32 devices in a mesh: seq: 8 (over z, y), head: 4 (over x, core).
Axes of the slice: x: 2, y: 2, z: 4, core: 2. Of those that a mesh axis runs over, the one named last changes fastest.
Arguments:
- tokens: bfloat16 [4096, 4096], P(('seq', 'head')), may hold values from -6 to 6
- w_keys: bfloat16 [4096, 256], P('seq', 'head'), may hold values from -0.09375 to 0.09375
- w_values: bfloat16 [8192, 4096], P('head', 'seq'), may hold values from -0.09375 to 0.09375
- w_out: bfloat16 [8192, 4096], P('head', 'seq'), may hold values from -0.0625 to 0.0625
- decay: float32 [64, 4096], P('head', 'seq'), may hold values from 0 to 1
- level_mix: float32 [64, 7, 4096], P('head', None, 'seq'), may hold values from 0 to 1
Outputs:
- result: bfloat16 [4096, 4096], P(('seq', 'head'))
The draws below stay inside these ranges and needn't reach their ends.
All inputs are finite; a program needn't handle non-finite values.
Results may differ from the reference program's by a relative error of at most 0.017.
Values may be sent and summed in bfloat16 or wider, within the bound.
A program may use at most 128 MiB of HBM per device.

```python
import math
import jax
import jax.numpy as jnp
from jax import lax

D = 4096
HEADS = 64
HEAD_DIM = 128
DS = 128
STRETCH = 64
LOCAL_LEVELS = 3
SEQ_LEVELS = 3
LEVELS = 7
TOK_DEV = 512
TOKENS = 4096
INNER = 8192
N_HEAD = 4


def draw_decay(key, part):
    pick_key, slow_key, fast_key, block_key, token_key = jax.random.split(key, 5)
    share = 0.5
    quick = jax.random.uniform(pick_key, (HEADS, 1)) < share
    slow_rate = jnp.exp(jax.random.uniform(slow_key, (HEADS, 1), minval=math.log(4e-05), maxval=math.log(0.0002)))
    fast_rate = jnp.exp(jax.random.uniform(fast_key, (HEADS, 1), minval=math.log(0.001), maxval=math.log(1.0 / 30.0)))
    base = jnp.where(quick, fast_rate, slow_rate)
    blocks = TOKENS // TOK_DEV
    block_factor = jnp.exp(jax.random.uniform(block_key, (HEADS, blocks, 1), minval=math.log(0.5), maxval=math.log(2.0)))
    block_factor = jnp.broadcast_to(block_factor, (HEADS, blocks, TOK_DEV)).reshape(HEADS, TOKENS)
    token_factor = jax.random.uniform(token_key, (HEADS, TOKENS), minval=0.5, maxval=2.0)
    return (base * block_factor * token_factor).astype(jnp.float32)


def draw_level_mix(key, part):
    level_id = jnp.arange(LEVELS)
    reach = STRETCH * 2.0 ** jnp.maximum(level_id - 1, 0)
    spread = jax.random.uniform(key, (HEADS, LEVELS, TOKENS), minval=0.3, maxval=0.9)
    return (spread / jnp.sqrt(reach)[None, :, None]).astype(jnp.float32)


def block_levels(key, extent, cuts, smallest, top_value):
    def one(axis_at, blocks):
        heights = jax.random.uniform(jax.random.fold_in(jax.random.fold_in(key, 6), axis_at), (blocks,), jnp.float32, smallest / len(cuts), top_value / len(cuts))
        return jnp.repeat(jnp.exp(heights), extent[axis_at] // blocks).reshape((-1,) + (1,) * (len(extent) - axis_at - 1))

    loudness = one(*cuts[0])
    for cut in cuts[1:]:
        loudness = loudness * one(*cut)
    return loudness


def bell_draw(rng, shape, scale, most, cuts=(), kind=jnp.bfloat16):
    factor_of = block_levels(rng, shape, cuts, -0.22, 0.18) if cuts else 1.0
    result = jax.random.normal(rng, shape, jnp.float32) * scale * factor_of
    return jnp.minimum(jnp.maximum(result, -most), most).astype(kind)


def setup_inputs(seed: int = 0) -> dict:
    seeds = jax.random.split(jax.random.key(seed), 7)
    tokens = bell_draw(seeds[0], (TOKENS, D), 1.0, 6.0, ((0, 32),))
    w_keys = bell_draw(seeds[1], (D, 2 * DS), D ** -0.5, 0.09375, ((0, 8), (1, 4)))
    w_values = bell_draw(seeds[2], (INNER, D), D ** -0.5, 0.09375, ((0, 4), (1, 8)))
    w_out = bell_draw(seeds[3], (INNER, D), INNER ** -0.5, 0.0625, ((0, 4), (1, 8)))
    decay = draw_decay(jax.random.fold_in(seeds[6], 71), 0)
    level_mix = draw_level_mix(jax.random.fold_in(seeds[6], 71), 0)
    return dict(tokens=tokens, w_keys=w_keys, w_values=w_values, w_out=w_out, decay=decay, level_mix=level_mix)


def level_of(query_stretch, key_stretch):
    differing = jnp.bitwise_xor(query_stretch, key_stretch)
    level_id = jnp.zeros(differing.shape, jnp.int32)
    for shift in range(LOCAL_LEVELS):
        level_id = level_id + (jnp.right_shift(differing, shift) > 0).astype(jnp.int32)
    return level_id

def near_block(query, keys, values3, cum_query, cum_keys, mix_query, first):
    rows = query.shape[0]
    key_count = keys.shape[0]
    score = lax.dot_general(query, keys, (((1,), (1,)), ((), ())), preferred_element_type=jnp.float32) / math.sqrt(DS)
    query_where = first + jnp.arange(rows, dtype=jnp.int32)
    key_where = jnp.arange(key_count, dtype=jnp.int32)
    causal = key_where[None, :] <= query_where[:, None]
    level_id = level_of(query_where[:, None] // STRETCH, key_where[None, :] // STRETCH)
    select = jnp.zeros((cum_query.shape[0], rows, key_count), jnp.float32)
    for level_index in range(LOCAL_LEVELS + 1):
        select = select + jnp.where(level_id == level_index, mix_query[:, level_index, :, None], jnp.float32(0.0))
    distance = jnp.maximum(cum_query[:, :, None] - cum_keys[:, None, :], 0.0)
    weight = jnp.where(causal, select * jnp.exp(-distance) * score, jnp.float32(0.0)).astype(jnp.bfloat16)
    return jnp.einsum('hts,shd->thd', weight.astype(jnp.float32), values3.astype(jnp.float32))

def reference(tokens, w_keys, w_values, w_out, decay, level_mix):
    key_query = jnp.dot(tokens, w_keys, preferred_element_type=jnp.float32).astype(jnp.bfloat16)
    query = key_query[:, :DS]
    keys = key_query[:, DS:]
    values = jnp.dot(tokens, w_values.T, preferred_element_type=jnp.float32).astype(jnp.bfloat16)
    blocks = TOKENS // TOK_DEV
    query_b = query.reshape(blocks, TOK_DEV, DS)
    keys_b = keys.reshape(blocks, TOK_DEV, DS)
    values_b = values.reshape(blocks, TOK_DEV, HEADS, HEAD_DIM)
    cum_b = jnp.cumsum(decay.reshape(HEADS, blocks, TOK_DEV), axis=2).transpose(1, 0, 2)
    mix_b = level_mix.reshape(HEADS, LEVELS, blocks, TOK_DEV).transpose(2, 0, 1, 3)
    spans = cum_b[:, :, -1]

    def own_state(packed):
        keys_one, values_one, cum_one = packed
        factor = jnp.exp(-(cum_one[:, -1:] - cum_one))
        decayed = (factor[:, :, None] * keys_one.astype(jnp.float32)[None]).astype(jnp.bfloat16)
        return jnp.einsum('hsk,shd->hkd', decayed.astype(jnp.float32), values_one.astype(jnp.float32))
    owns = lax.map(own_state, (keys_b, values_b, cum_b))
    running = jnp.cumsum(spans, axis=0)
    block_ids = jnp.arange(blocks, dtype=jnp.int32)

    def one_block(packed):
        index, query_one, keys_one, values_one, cum_one, mix_one = packed
        near = near_block(query_one, keys_one, values_one, cum_one, cum_one, mix_one, 0)
        far = jnp.zeros_like(near)
        query32 = query_one.astype(jnp.float32)
        for bit in range(SEQ_LEVELS):
            upper = jnp.bitwise_and(jnp.right_shift(index, bit), 1) == 1
            base = jnp.left_shift(jnp.right_shift(index, bit + 1), bit + 1)
            last = base + (1 << bit) - 1
            inside = (block_ids >= base) & (block_ids <= last)
            end_sum = running[last]
            spread = jnp.where(inside[:, None], jnp.exp(-jnp.maximum(end_sum[None, :] - running, 0.0)), jnp.float32(0.0))
            bucket = jnp.einsum('mh,mhkd->hkd', spread, owns, precision=lax.Precision.HIGHEST)
            between = jnp.maximum(running[jnp.maximum(index - 1, 0)] - end_sum, 0.0)
            coef = jnp.where(upper, mix_one[:, LOCAL_LEVELS + 1 + bit, :] * jnp.exp(-(between[:, None] + cum_one)) / math.sqrt(DS), jnp.float32(0.0))
            reach = jnp.einsum('tk,hkd->thd', query32, bucket, precision=lax.Precision.HIGHEST)
            far = far + coef.T[:, :, None] * reach
        return near + far
    mixed = lax.map(one_block, (block_ids, query_b, keys_b, values_b, cum_b, mix_b))
    mixed = mixed.reshape(TOKENS, HEADS * HEAD_DIM).astype(jnp.bfloat16)
    group = HEADS * HEAD_DIM // N_HEAD

    def add_group(index, total):
        start = (jnp.asarray(index).astype(jnp.int32) * group).astype(jnp.int32)
        columns = lax.dynamic_slice_in_dim(mixed, start, group, 1)
        weights = lax.dynamic_slice_in_dim(w_out, start, group, 0)
        partial_out = jnp.dot(columns, weights, preferred_element_type=jnp.float32).astype(jnp.bfloat16)
        return total + partial_out.astype(jnp.float32)
    summed = lax.fori_loop(0, N_HEAD, add_group, jnp.zeros((TOKENS, D), jnp.float32))
    return summed.astype(jnp.bfloat16)
```

```python
import math

import jax
import jax.numpy as jnp
from jax import lax
from jax.sharding import PartitionSpec as P

HEAD_DIM = 128
DS = 128
STRETCH = 64
LOCAL_LEVELS = 3
PAIR_BIT = 1


def swap(x, axis, bit):
    return lax.ppermute(x, axis, [(i, i ^ (1 << bit)) for i in range(lax.axis_size(axis))])


def bits_of(axis):
    return lax.axis_size(axis).bit_length() - 1


def bit_at(index, bit):
    return jnp.bitwise_and(jnp.right_shift(index, bit), 1)


def half(x, which, axis):
    size = x.shape[axis] // 2
    return lax.dynamic_slice_in_dim(x, which * size, size, axis)


def join(mine, other, upper, axis):
    return jnp.where(
        upper == 1,
        jnp.concatenate([other, mine], axis),
        jnp.concatenate([mine, other], axis),
    )


def level_of(query_stretch, key_stretch):
    differing = jnp.bitwise_xor(query_stretch, key_stretch)
    level_id = jnp.zeros(differing.shape, jnp.int32)
    for shift in range(LOCAL_LEVELS):
        level_id = level_id + (jnp.right_shift(differing, shift) > 0).astype(jnp.int32)
    return level_id


def far_pieces(keep, other, bits):
    pieces = [(0, keep), (1 << PAIR_BIT, swap(other, "seq", PAIR_BIT))]
    for bit in range(PAIR_BIT + 1, bits):
        pieces = pieces + [(e | 1 << bit, swap(p, "seq", bit)) for e, p in pieces]
    return pieces


def local(tokens, w_keys, w_values, w_out, decay, level_mix):
    seq = lax.axis_index("seq")
    head = lax.axis_index("head")
    bits = bits_of("seq")
    head_bits = bits_of("head")
    pair = bit_at(seq, PAIR_BIT)
    low = bit_at(seq, 0)
    block_rows = decay.shape[1]
    width = w_values.shape[1]
    features = tokens.shape[1]

    whole = tokens.reshape((1,) * (head_bits + 1) + tokens.shape)
    whole = join(whole, swap(whole, "seq", PAIR_BIT), pair, 0)
    for bit in reversed(range(head_bits)):
        whole = join(whole, swap(whole, "head", bit), bit_at(head, bit), head_bits - bit)
    whole = whole.reshape(2 * block_rows, features)

    key_pieces = [(0, w_keys)]
    for bit in range(bits):
        key_pieces = key_pieces + [(e | 1 << bit, swap(p, "seq", bit)) for e, p in key_pieces]
    all_keys = jnp.zeros((features, w_keys.shape[1]), w_keys.dtype)
    for e, p in key_pieces:
        all_keys = lax.dynamic_update_slice_in_dim(
            all_keys, p, jnp.bitwise_xor(seq, e) * p.shape[0], 0
        )
    key_query = jnp.dot(whole, all_keys, preferred_element_type=jnp.float32).astype(jnp.bfloat16)
    for bit in range(head_bits):
        key_query = join(key_query, swap(key_query, "head", bit), bit_at(head, bit), 1)
    query = key_query[:, :DS].reshape(2, block_rows, DS)
    keys = key_query[:, DS:].reshape(2, block_rows, DS)

    value_pieces = far_pieces(half(w_values, pair, 0), half(w_values, 1 - pair, 0), bits)
    values = None
    for e, p in value_pieces:
        both = join(p, swap(p, "seq", 0), low, 1)
        at = jnp.bitwise_xor(jnp.right_shift(seq, 1), e >> 1) * (2 * width)
        columns = lax.dynamic_slice_in_dim(whole, at, 2 * width, 1)
        term = lax.dot_general(
            columns, both, (((1,), (1,)), ((), ())), preferred_element_type=jnp.float32
        )
        values = term if values is None else values + term
    values = values.astype(jnp.bfloat16)
    heads = decay.shape[0] // 2
    values4 = values.reshape(2, block_rows, heads, HEAD_DIM)

    decay2 = join(
        half(decay, pair, 0)[None], swap(half(decay, 1 - pair, 0), "seq", PAIR_BIT)[None], pair, 0
    )
    mix = join(
        half(level_mix, pair, 0)[None],
        swap(half(level_mix, 1 - pair, 0), "seq", PAIR_BIT)[None],
        pair,
        0,
    )
    cum = jnp.cumsum(decay2, axis=2)
    span = cum[:, :, -1]

    score = jnp.einsum(
        "btk,bsk->bts", query, keys, preferred_element_type=jnp.float32
    ) / math.sqrt(DS)
    where = jnp.arange(block_rows, dtype=jnp.int32)
    causal = where[None, :] <= where[:, None]
    level_id = level_of(where[:, None] // STRETCH, where[None, :] // STRETCH)
    select = jnp.zeros((2, heads, block_rows, block_rows), jnp.float32)
    for level_index in range(LOCAL_LEVELS + 1):
        select = select + jnp.where(
            level_id == level_index, mix[:, :, level_index, :, None], jnp.float32(0.0)
        )
    distance = jnp.maximum(cum[:, :, :, None] - cum[:, :, None, :], 0.0)
    weight = jnp.where(
        causal, select * jnp.exp(-distance) * score[:, None], jnp.float32(0.0)
    ).astype(jnp.bfloat16)
    near = jnp.einsum("bhts,bshd->bthd", weight, values4, preferred_element_type=jnp.float32)

    factor = jnp.exp(-(span[:, :, None] - cum))
    decayed = (factor[:, :, :, None] * keys.astype(jnp.float32)[:, None]).astype(jnp.bfloat16)
    state = jnp.einsum("bhsk,bshd->bhkd", decayed, values4, preferred_element_type=jnp.float32)
    total = span
    before = jnp.zeros_like(span)
    block_ids = jnp.array([0, 1], jnp.int32) * (1 << PAIR_BIT) + (seq - pair * (1 << PAIR_BIT))
    far = jnp.zeros((2, block_rows, heads, HEAD_DIM), jnp.float32)
    for bit in range(bits):
        sent, sent_span = state.astype(jnp.bfloat16), total
        if bit == PAIR_BIT:
            partner, partner_span = sent[::-1], sent_span[::-1]
        else:
            partner, partner_span = swap(sent, "seq", bit), swap(sent_span, "seq", bit)
        upper = (bit_at(block_ids, bit) == 1)[:, None]
        coef = jnp.where(
            upper[:, :, None],
            mix[:, :, LOCAL_LEVELS + 1 + bit, :]
            * jnp.exp(-(before[:, :, None] + cum))
            / math.sqrt(DS),
            jnp.float32(0.0),
        )
        reach = jnp.einsum("btk,bhkd->bthd", query, partner, preferred_element_type=jnp.float32)
        far = far + coef.transpose(0, 2, 1)[:, :, :, None] * reach
        if bit < bits - 1:
            partner32 = partner.astype(jnp.float32)
            state = jnp.where(
                upper[:, :, None, None],
                jnp.exp(-total)[:, :, None, None] * partner32 + state,
                jnp.exp(-partner_span)[:, :, None, None] * state + partner32,
            )
            before = jnp.where(upper, before + partner_span, before)
            total = total + partner_span
    mixed = (near + far).reshape(2 * block_rows, heads * HEAD_DIM).astype(jnp.bfloat16)

    result = jnp.zeros((tokens.shape[0], features), jnp.bfloat16)
    out_pieces = far_pieces(half(w_out, pair, 0), half(w_out, 1 - pair, 0), bits)
    kept, given = {}, {}
    for e, p in out_pieces:
        both = join(p, swap(p, "seq", 0), low, 1)
        part = jnp.dot(mixed, both, preferred_element_type=jnp.float32).astype(jnp.bfloat16)
        part = part.reshape((2,) + (2,) * head_bits + (tokens.shape[0], both.shape[1]))
        for bit in range(head_bits):
            axis = head_bits - bit
            mine = bit_at(head, bit)
            own = lax.dynamic_index_in_dim(part, mine, axis, keepdims=True)
            got = swap(lax.dynamic_index_in_dim(part, 1 - mine, axis, keepdims=True), "head", bit)
            part = (own.astype(jnp.float32) + got.astype(jnp.float32)).astype(jnp.bfloat16)
        kept[e] = lax.dynamic_index_in_dim(part, pair, 0, keepdims=True)
        given[e] = lax.dynamic_index_in_dim(part, 1 - pair, 0, keepdims=True)
    for e, own in kept.items():
        got = swap(given[e ^ 1 << PAIR_BIT], "seq", PAIR_BIT)
        done = (own.astype(jnp.float32) + got.astype(jnp.float32)).astype(jnp.bfloat16)
        at = jnp.bitwise_xor(jnp.right_shift(seq, 1), e >> 1) * (2 * width)
        result = lax.dynamic_update_slice_in_dim(
            result, done.reshape(tokens.shape[0], 2 * width), at, 1
        )
    return result


def solution(mesh):
    placed = (
        P(("seq", "head"), None),
        P("seq", "head"),
        P("head", "seq"),
        P("head", "seq"),
        P("head", "seq"),
        P("head", None, "seq"),
    )
    return jax.shard_map(
        local, mesh=mesh, in_specs=placed, out_specs=P(("seq", "head"), None), check_vma=False
    )
```

```python
import math

import jax
import jax.numpy as jnp
from jax import lax
from jax.sharding import PartitionSpec as P


HEAD_DIM = 128
DS = 128
STRETCH = 64
LOCAL_LEVELS = 3
PAIR_BIT = 1


def ppermute_bit(x, axis, bit):
    return lax.ppermute(x, axis, [(i, i ^ (1 << bit)) for i in range(lax.axis_size(axis))])


def bits_of(axis):
    return lax.axis_size(axis).bit_length() - 1


def bit_at(index, bit):
    return jnp.bitwise_and(jnp.right_shift(index, bit), 1)


def half(x, which, axis):
    size = x.shape[axis] // 2
    return lax.dynamic_slice_in_dim(x, which * size, size, axis)


def join(mine, other, upper, axis):
    return jnp.where(
        upper == 1,
        jnp.concatenate([other, mine], axis),
        jnp.concatenate([mine, other], axis),
    )


def level_of(query_stretch, key_stretch):
    differing = jnp.bitwise_xor(query_stretch, key_stretch)
    level_id = jnp.zeros(differing.shape, jnp.int32)
    for shift in range(LOCAL_LEVELS):
        level_id = level_id + (jnp.right_shift(differing, shift) > 0).astype(jnp.int32)
    return level_id


def far_pieces(keep, other, bits):
    pieces = [(0, keep), (1 << PAIR_BIT, ppermute_bit(other, "seq", PAIR_BIT))]
    for bit in range(PAIR_BIT + 1, bits):
        pieces = pieces + [(e | 1 << bit, ppermute_bit(p, "seq", bit)) for e, p in pieces]
    return pieces


def local(tokens, w_keys, w_values, w_out, decay, level_mix):
    seq = lax.axis_index("seq")
    head = lax.axis_index("head")
    bits = bits_of("seq")
    head_bits = bits_of("head")
    pair = bit_at(seq, PAIR_BIT)
    low = bit_at(seq, 0)
    block_rows = decay.shape[1]
    width = w_values.shape[1]
    features = tokens.shape[1]

    parts = [tokens.reshape((1,) * (head_bits + 1) + tokens.shape)]
    parts.append(ppermute_bit(parts[0], "seq", PAIR_BIT))
    for which in range(2):
        for bit in reversed(range(head_bits)):
            got = ppermute_bit(parts[which], "head", bit)
            parts[which] = join(parts[which], got, bit_at(head, bit), head_bits - bit)
    whole = join(parts[0], parts[1], pair, 0)
    whole = whole.reshape(2 * block_rows, features)

    key_pieces = [(0, w_keys)]
    for bit in range(bits):
        key_pieces = key_pieces + [(e | 1 << bit, ppermute_bit(p, "seq", bit)) for e, p in key_pieces]
    all_keys = jnp.zeros((features, w_keys.shape[1]), w_keys.dtype)
    for e, p in key_pieces:
        all_keys = lax.dynamic_update_slice_in_dim(
            all_keys, p, jnp.bitwise_xor(seq, e) * p.shape[0], 0
        )
    key_query = jnp.dot(whole, all_keys, preferred_element_type=jnp.float32).astype(jnp.bfloat16)
    for bit in range(head_bits):
        key_query = join(key_query, ppermute_bit(key_query, "head", bit), bit_at(head, bit), 1)
    query = key_query[:, :DS].reshape(2, block_rows, DS)
    keys = key_query[:, DS:].reshape(2, block_rows, DS)

    value_pieces = far_pieces(half(w_values, pair, 0), half(w_values, 1 - pair, 0), bits)
    values = None
    for e, p in value_pieces:
        both = join(p, ppermute_bit(p, "seq", 0), low, 1)
        at = jnp.bitwise_xor(jnp.right_shift(seq, 1), e >> 1) * (2 * width)
        columns = lax.dynamic_slice_in_dim(whole, at, 2 * width, 1)
        term = lax.dot_general(
            columns, both, (((1,), (1,)), ((), ())), preferred_element_type=jnp.float32
        )
        values = term if values is None else values + term
    values = values.astype(jnp.bfloat16)
    heads = decay.shape[0] // 2
    values4 = values.reshape(2, block_rows, heads, HEAD_DIM)

    decay2 = join(
        half(decay, pair, 0)[None], ppermute_bit(half(decay, 1 - pair, 0), "seq", PAIR_BIT)[None], pair, 0
    )
    mix = join(
        half(level_mix, pair, 0)[None],
        ppermute_bit(half(level_mix, 1 - pair, 0), "seq", PAIR_BIT)[None],
        pair,
        0,
    )
    cum = jnp.cumsum(decay2, axis=2)
    span = cum[:, :, -1]

    score = jnp.einsum(
        "btk,bsk->bts", query, keys, preferred_element_type=jnp.float32
    ) / math.sqrt(DS)
    where = jnp.arange(block_rows, dtype=jnp.int32)
    causal = where[None, :] <= where[:, None]
    level_id = level_of(where[:, None] // STRETCH, where[None, :] // STRETCH)
    select = jnp.zeros((2, heads, block_rows, block_rows), jnp.float32)
    for level_index in range(LOCAL_LEVELS + 1):
        select = select + jnp.where(
            level_id == level_index, mix[:, :, level_index, :, None], jnp.float32(0.0)
        )
    distance = jnp.maximum(cum[:, :, :, None] - cum[:, :, None, :], 0.0)
    weight = jnp.where(
        causal, select * jnp.exp(-distance) * score[:, None], jnp.float32(0.0)
    ).astype(jnp.bfloat16)
    near = jnp.einsum("bhts,bshd->bthd", weight, values4, preferred_element_type=jnp.float32)

    factor = jnp.exp(-(span[:, :, None] - cum))
    decayed = (factor[:, :, :, None] * keys.astype(jnp.float32)[:, None]).astype(jnp.bfloat16)
    state = jnp.einsum("bhsk,bshd->bhkd", decayed, values4, preferred_element_type=jnp.float32)
    total = span
    before = jnp.zeros_like(span)
    block_ids = jnp.array([0, 1], jnp.int32) * (1 << PAIR_BIT) + (seq - pair * (1 << PAIR_BIT))
    far = jnp.zeros((2, block_rows, heads, HEAD_DIM), jnp.float32)
    for bit in range(bits):
        sent, sent_span = state.astype(jnp.bfloat16), total
        if bit == PAIR_BIT:
            partner, partner_span = sent[::-1], sent_span[::-1]
        else:
            partner, partner_span = ppermute_bit(sent, "seq", bit), ppermute_bit(sent_span, "seq", bit)
        upper = (bit_at(block_ids, bit) == 1)[:, None]
        coef = jnp.where(
            upper[:, :, None],
            mix[:, :, LOCAL_LEVELS + 1 + bit, :]
            * jnp.exp(-(before[:, :, None] + cum))
            / math.sqrt(DS),
            jnp.float32(0.0),
        )
        reach = jnp.einsum("btk,bhkd->bthd", query, partner, preferred_element_type=jnp.float32)
        far = far + coef.transpose(0, 2, 1)[:, :, :, None] * reach
        if bit < bits - 1:
            partner32 = partner.astype(jnp.float32)
            state = jnp.where(
                upper[:, :, None, None],
                jnp.exp(-total)[:, :, None, None] * partner32 + state,
                jnp.exp(-partner_span)[:, :, None, None] * state + partner32,
            )
            before = jnp.where(upper, before + partner_span, before)
            total = total + partner_span
    mixed = (near + far).reshape(2 * block_rows, heads * HEAD_DIM).astype(jnp.bfloat16)

    result = jnp.zeros((tokens.shape[0], features), jnp.bfloat16)
    out_pieces = far_pieces(half(w_out, pair, 0), half(w_out, 1 - pair, 0), bits)
    kept, given = {}, {}
    for e, p in out_pieces:
        both = join(p, ppermute_bit(p, "seq", 0), low, 1)
        part = jnp.dot(mixed, both, preferred_element_type=jnp.float32).astype(jnp.bfloat16)
        part = part.reshape((2,) + (2,) * head_bits + (tokens.shape[0], both.shape[1]))
        for bit in range(head_bits):
            axis = head_bits - bit
            mine = bit_at(head, bit)
            own = lax.dynamic_index_in_dim(part, mine, axis, keepdims=True)
            got = ppermute_bit(lax.dynamic_index_in_dim(part, 1 - mine, axis, keepdims=True), "head", bit)
            part = (own.astype(jnp.float32) + got.astype(jnp.float32)).astype(jnp.bfloat16)
        kept[e] = lax.dynamic_index_in_dim(part, pair, 0, keepdims=True)
        given[e] = lax.dynamic_index_in_dim(part, 1 - pair, 0, keepdims=True)
    for e, own in kept.items():
        got = ppermute_bit(given[e ^ 1 << PAIR_BIT], "seq", PAIR_BIT)
        done = (own.astype(jnp.float32) + got.astype(jnp.float32)).astype(jnp.bfloat16)
        at = jnp.bitwise_xor(jnp.right_shift(seq, 1), e >> 1) * (2 * width)
        result = lax.dynamic_update_slice_in_dim(
            result, done.reshape(tokens.shape[0], 2 * width), at, 1
        )
    return result


def solution(mesh):
    placed = (
        P(("seq", "head"), None),
        P("seq", "head"),
        P("head", "seq"),
        P("head", "seq"),
        P("head", "seq"),
        P("head", None, "seq"),
    )

    return jax.shard_map(
        local, mesh=mesh, in_specs=placed, out_specs=P(("seq", "head"), None), check_vma=False
    )
```
